32 devices in a mesh: lang: 2 (over y), clu: 16 (over z, x, core).
Axes of the slice: x: 2, y: 2, z: 4, core: 2. Of those that a mesh axis runs over, the one named last changes fastest.
Arguments:
- embeddings: bfloat16 [8192, 1024], P(('lang', 'clu')), parts along dimension 0, may hold values from -6 to 6
- assignment: int32 [8192, 1], P(('lang', 'clu')), parts along dimension 0, may hold values from 0 to 31; in each aligned block of 256 rows (0 to 255, 256 to 511, ...) at most 16 rows name the same one
Outputs:
- best_similarity: float32 [8192], P(('lang', 'clu')), parts along dimension 0
The draws below stay inside these ranges and needn't reach their ends.
There are 2 independent parts, one for each index of `lang`. The reference program is written for one: setup_inputs(seed, part) draws one part's arguments, and reference() takes and returns one part's arrays. A program takes and returns all parts, laid end to end along the dimension named above; each array names one. Nothing has to cross between parts.
Inputs may be any that keep to these rules, and one draw needn't show every extreme that they name: `assignment`: in each aligned block of 256 rows (the rows of one device) no cluster is named by more than 16 rows; every cluster is named by some row.
All inputs are finite; a program needn't handle non-finite values.
Results may differ from the reference program's by a relative error of at most 0.0016.
Values may be sent and summed in bfloat16 or wider, within the bound.
A program may use at most 64 MiB of HBM per device.

```python
import math
import jax
import jax.numpy as jnp
import numpy as np
from jax import lax

D = 1024
ROWS_DEV = 256
CLUSTERS = 32
MOST = 16
ROWS = 4096
N_CLU = 16


def shard_levels(rng, extent, shards, least, top_value):
    level = 1.0
    for dim, blocks in shards:
        draws = jax.random.uniform(jax.random.fold_in(jax.random.fold_in(rng, 6), dim), (blocks,), jnp.float32, least / len(shards), top_value / len(shards))
        level = level * jnp.repeat(jnp.exp(draws), extent[dim] // blocks).reshape((-1,) + (1,) * (len(extent) - 1 - dim))
    return level


def deal_out(rng, own, number, rows, amount, top, most, skew):
    ranking = jax.random.permutation(rng, amount)
    crowded, common = portions_of(amount, rows * top, most, skew, True), portions_of(amount, rows * top, most, skew, False)
    places = jnp.arange(amount)

    def named(sizes, turn):
        used = int((sizes > 0).sum())
        fixed = max(1, used // 4)
        moved = fixed + (places - fixed + turn * (used - fixed)) % max(1, amount - fixed)
        return jnp.zeros((amount,), jnp.int32).at[ranking[jnp.where(places < fixed, places, moved)]].set(jnp.asarray(sizes, jnp.int32))

    sizes = jnp.where(number % 4 == 0, named(crowded, number // 4), named(common, number - number // 4 - 1))
    mixed = jax.random.permutation(jax.random.fold_in(own, 3), amount)
    donor, taker = mixed[0:amount // 2 * 2:2], mixed[1:amount // 2 * 2:2]
    margin = jnp.minimum(sizes[donor] - 1, most - sizes[taker]) // 2
    margin = jnp.where((donor == ranking[0]) | (taker == ranking[0]) | (sizes[taker] == 0), 0, jnp.maximum(margin, 0))
    moved = jax.random.randint(jax.random.fold_in(own, 4), (amount // 2,), 0, 1 << 20) % (margin + 1)
    sizes = sizes.at[donor].add(-moved).at[taker].add(moved)
    items = jnp.searchsorted(jnp.cumsum(sizes), jnp.arange(rows * top), side="right").astype(jnp.int32)
    table = items.reshape(top, rows).T
    table = table[jax.random.permutation(jax.random.fold_in(own, 1), rows)]
    turn = jax.random.randint(jax.random.fold_in(own, 2), (rows, 1), 0, top)
    return jnp.take_along_axis(table, (jnp.arange(top)[None, :] + turn) % top, axis=1)


def portions_of(number_of, total, reach, slope, full):
    weights = [(1 << 20) // math.isqrt(standing ** slope) + 1 for standing in range(1, number_of + 1)]
    largest = reach if full else min(reach, max(-(-total // number_of), total * weights[0] // sum(weights)))
    least = 1 if total - largest >= number_of - 1 else 0
    holding, surplus = [largest] + [least] * (number_of - 1), total - largest - least * (number_of - 1)
    while surplus > 0:
        movable = [i for i in range(1, number_of) if holding[i] < largest] or [i for i in range(1, number_of) if holding[i] < reach]
        mass, budget = sum([weights[i] for i in movable]), surplus
        for i in movable:
            extra = min(reach - holding[i], max(1, budget * weights[i] // mass), surplus)
            holding[i] = holding[i] + extra
            surplus = surplus - extra
    return np.array(holding)


def bell_draw(own_key, dims, deviation, most, pieces=(), kind=jnp.bfloat16):
    gain = shard_levels(own_key, dims, pieces, -0.22, 0.18) if pieces else 1.0
    drawn = jax.random.normal(own_key, dims, jnp.float32) * deviation * gain
    return jnp.minimum(jnp.maximum(drawn, -most), most).astype(kind)


def setup_inputs(seed: int = 0, part: int = 0) -> dict:
    splits = jax.random.split(jax.random.key(seed), 3)
    part_splits = jax.random.split(jax.random.fold_in(splits[2], part), 3)
    embeddings = bell_draw(part_splits[0], (ROWS, D), 1.0, 6.0, ((0, 16),))
    assignment_keys = jax.random.split(jax.random.fold_in(part_splits[1], 1), ROWS // ROWS_DEV)
    assignment_turns = jax.random.permutation(jax.random.fold_in(part_splits[1], 3), ROWS // ROWS_DEV)
    assignment = jax.vmap(lambda own, number: deal_out(jax.random.fold_in(part_splits[1], 2), own, number, ROWS_DEV, CLUSTERS, 1, MOST, 2))(assignment_keys, assignment_turns).reshape((ROWS, 1))
    return {"embeddings": embeddings, "assignment": assignment}


EPS = 1e-06

def normalize(embeddings):
    values = embeddings.astype(jnp.float32)
    scale = lax.rsqrt(lax.optimization_barrier(jnp.sum(values * values, axis=-1, keepdims=True)) + EPS)
    return (values * scale).astype(jnp.bfloat16)

def reference(embeddings, assignment):
    unit = normalize(embeddings)
    cluster = assignment[:, 0].astype(jnp.int32)
    total = cluster.shape[0]
    order = jnp.argsort(cluster, stable=True).astype(jnp.int32)
    ranked = cluster[order]
    labels = jnp.arange(CLUSTERS, dtype=jnp.int32)
    starts = jnp.searchsorted(ranked, labels, side='left').astype(jnp.int32)
    ends = jnp.searchsorted(ranked, labels, side='right').astype(jnp.int32)
    sorted_unit = unit[order]
    width = N_CLU * MOST
    offsets = jnp.arange(width, dtype=jnp.int32)
    distinct = offsets[:, None] != offsets[None, :]

    def score(label):
        index = jnp.clip(starts[label] + offsets, 0, total - 1).astype(jnp.int32)
        live = offsets < ends[label] - starts[label]
        rows = sorted_unit[index]
        gram = jnp.dot(rows, rows.T, preferred_element_type=jnp.float32)
        keep = distinct & live[None, :]
        best = lax.optimization_barrier(jnp.max(jnp.where(keep, gram, jnp.float32(-2.0)), axis=1))
        return jnp.maximum(best, jnp.float32(-1.0))
    table = lax.map(score, labels)
    position = jnp.arange(total, dtype=jnp.int32)
    inside = (position - starts[ranked]).astype(jnp.int32)
    sorted_best = table[ranked, inside]
    return jnp.zeros((total,), jnp.float32).at[order].set(sorted_best)
```

```python
import functools

import jax
import jax.numpy as jnp
from jax import lax
from jax.experimental import pallas as pl
from jax.experimental.pallas import tpu as pltpu
from jax.sharding import PartitionSpec as P

CLU_DEV = 2
LANES = 128
EPS = 1e-06
DEAD = 16.0
ALIVE = 8.0
LOWEST = -1e30
SIDE = 2


def normalize(embeddings):
    values = embeddings.astype(jnp.float32)
    scale = lax.rsqrt(jnp.sum(values * values, axis=-1, keepdims=True) + EPS)
    return (values * scale).astype(jnp.bfloat16)


def exchange_kernel(
    groups, most, emb_ref, cluster_ref, out_ref,
    raw, cluster_in, outgoing, arrived, fence, best, result, returned,
    load_sem, cluster_sem, send_sem, recv_sem, back_send_sem, back_recv_sem, ready,
):
    count, width = raw.shape
    block = CLU_DEV * most
    total = groups * block
    batch = LANES // block
    parts = groups // batch
    half, quarter = groups // 2, groups // 4
    me = lax.axis_index("clu")
    inner = ((me // half) ^ (me // quarter)) & 1
    outer = 1 - inner

    barrier = pltpu.get_barrier_semaphore()
    near = [k for k in range(1, groups) if k & SIDE == 0] + [SIDE]
    for k in near:
        pl.semaphore_signal(
            barrier, inc=1, device_id={"clu": me ^ k},
            device_id_type=pl.DeviceIdType.MESH,
        )
    load_cluster = pltpu.make_async_copy(cluster_ref, cluster_in, cluster_sem)
    load_cluster.start()
    load = pltpu.make_async_copy(emb_ref, raw, load_sem)
    load.start()

    def sent_to(p):
        return p if p < half else p ^ (quarter * outer)

    def landed_from(p):
        return p if p < half else p ^ SIDE

    def piece_of(p):
        if p < total // block - batch:
            return p // batch
        return parts - 1 + (p - (groups - batch)) // (batch // 2)

    def send(p):
        k = sent_to(p)
        peer = me ^ k
        if p < half:
            place, sem = p, piece_of(p)
        else:
            low, top = (p ^ SIDE) % quarter, (p // quarter % 2) ^ outer
            place = half + quarter * top + low
            sem = jnp.where(top == 1, piece_of(half + quarter + low), piece_of(half + low))
        return pltpu.make_async_remote_copy(
            src_ref=outgoing.at[pl.ds(p * block, block)],
            dst_ref=arrived.at[pl.ds(pl.multiple_of(place * block, block), block)],
            send_sem=send_sem,
            recv_sem=recv_sem.at[sem],
            device_id={"clu": peer},
            device_id_type=pl.DeviceIdType.MESH,
        )

    def receive(start, stop):
        rows = pl.ds(start * block, (stop - start) * block)
        return pltpu.make_async_remote_copy(
            src_ref=outgoing.at[rows],
            dst_ref=arrived.at[rows],
            send_sem=send_sem,
            recv_sem=recv_sem.at[piece_of(start)],
            device_id={"clu": me ^ SIDE},
            device_id_type=pl.DeviceIdType.MESH,
        )

    def peer_of(cluster):
        return (cluster // CLU_DEV) ^ me

    def slot_of(cluster, rank):
        peer = peer_of(cluster)
        peer = jnp.where(peer >= half, peer ^ (quarter * outer), peer)
        return peer * block + (cluster % CLU_DEV) * most + rank

    row_id = lax.broadcasted_iota(jnp.int32, (count, count), 0)
    col_id = lax.broadcasted_iota(jnp.int32, (count, count), 1)
    first = lax.broadcasted_iota(jnp.int32, (count, LANES), 1) == 0
    mark = jnp.where(first, DEAD, 0.0).astype(jnp.bfloat16)
    blank = jnp.where(
        lax.broadcasted_iota(jnp.int32, (LANES, LANES), 1) == 0, DEAD, 0.0
    )
    load_cluster.wait()
    cluster_row = cluster_in[...]
    spread = jnp.broadcast_to(cluster_row, (count, count))
    cluster_col = jnp.sum(
        jnp.where(row_id == col_id, spread, 0), axis=1, keepdims=True
    )
    same = cluster_col == spread
    rank_row = jnp.sum(
        jnp.where(same & (row_id < col_id), 1, 0), axis=0, keepdims=True
    )
    slot_row = jnp.broadcast_to(slot_of(cluster_row, rank_row), (LANES, count))

    def pack(g):
        rows = pl.ds(g * LANES, LANES)
        hit = lax.broadcasted_iota(jnp.int32, (LANES, count), 0) + g * LANES == slot_row
        place = jnp.where(hit, 1.0, 0.0).astype(jnp.bfloat16)
        packed = jnp.dot(place, raw[...], preferred_element_type=jnp.float32)
        used = jnp.dot(place, mark, preferred_element_type=jnp.float32)
        outgoing[rows, LANES:width] = packed[:, LANES:width].astype(jnp.bfloat16)
        outgoing[rows, 0:LANES] = (packed[:, 0:LANES] + (blank - used)).astype(jnp.bfloat16)

    def members(g, side):
        span = range(max(1, g * batch), (g + 1) * batch)
        return [p for p in span if (p & SIDE != 0) == side]

    far = parts // 2
    load.wait()
    pack(far)
    pl.semaphore_wait(barrier, len(near))
    pl.semaphore_signal(
        ready, inc=1, device_id={"clu": me ^ SIDE},
        device_id_type=pl.DeviceIdType.MESH,
    )

    @pl.when(inner == 1)
    def _():
        for p in members(far, False):
            send(p).start()

    for g in range(far - 1, 0, -1):
        pack(g)

    @pl.when(outer == 1)
    def _():
        for g in range(far - 1, 0, -1):
            for p in members(g, False):
                send(p).start()
        for p in members(far, False):
            send(p).start()

    pl.semaphore_wait(ready, 1)

    @pl.when(inner == 1)
    def _():
        for p in members(far, True):
            send(p).start()

    @pl.when(outer == 1)
    def _():
        for g in range(far - 1, 0, -1):
            for p in members(g, True):
                send(p).start()
        for p in members(far, True):
            send(p).start()

    raw[...] = normalize(raw[...])
    pack(0)
    for p in members(0, True) + members(0, False):
        send(p).start()
    for g in range(far + 1, parts):
        pack(g)
        for p in members(g, True) + members(g, False):
            send(p).start()
    arrived[0:block, :] = outgoing[0:block, :]

    rank_col = jnp.sum(
        jnp.where(same & (col_id < row_id), 1, 0), axis=1, keepdims=True
    )
    peer_col = peer_of(cluster_col)
    lane_peer = jnp.where(peer_col >= half, peer_col ^ SIDE, peer_col)
    lane_col = lane_peer % batch * block + cluster_col % CLU_DEV * most + rank_col
    chosen = lax.broadcasted_iota(jnp.int32, (count, LANES), 1) == lane_col
    best[...] = jnp.full((total, LANES), -1.0, jnp.float32)

    def score(start, stop):
        low, high = start * block, stop * block
        wide = high - low
        lead = arrived[low:high, 0:LANES].astype(jnp.float32)
        lane = lax.broadcasted_iota(jnp.int32, (wide, LANES), 1)
        row = lax.broadcasted_iota(jnp.int32, (wide, LANES), 0)
        void = jnp.where((lane == 0) & (lead > ALIVE), 1.0, 0.0).astype(jnp.bfloat16)
        ones = jnp.full((LANES, LANES), 1.0, jnp.bfloat16)
        void_col = jnp.dot(void, ones, preferred_element_type=jnp.float32)
        void_row = lax.dot_general(
            ones[0:16], void, (((1,), (1,)), ((), ())), preferred_element_type=jnp.float32
        )[0:1]
        apart = ((row ^ lane) & most) != 0
        fence[low:high, :] = jnp.where(apart | (void_col > 0.5), LOWEST, 0.0)

        if batch <= start < half:
            arrived[low:high, :] = normalize(arrived[low:high, :])
        elif start >= half:
            @pl.when(outer == 1)
            def _():
                arrived[low:high, :] = normalize(arrived[low:high, :])

        gram = lax.dot_general(
            arrived[0:high, :], arrived[low:high, :], (((1,), (1,)), ((), ())),
            preferred_element_type=jnp.float32,
        )
        gram = gram + fence[0:high, 0:wide]
        self_row = lax.broadcasted_iota(jnp.int32, (wide, wide), 0)
        self_col = lax.broadcasted_iota(jnp.int32, (wide, wide), 1)
        own = jnp.where(self_row == self_col, LOWEST, gram[low:high])
        by_col = jnp.max(own, axis=0, keepdims=True)
        bias = void_row * LOWEST
        best[low:high, 0:wide] = jnp.maximum(best[low:high, 0:wide], own + bias)
        if low:
            old = gram[0:low]
            by_col = jnp.maximum(by_col, jnp.max(old, axis=0, keepdims=True))
            best[0:low, 0:wide] = jnp.maximum(best[0:low, 0:wide], old + bias)
        result[0, :, low:high] = by_col

    mid = groups - batch // 2
    pieces = [(g * batch, (g + 1) * batch) for g in range(parts - 1)]
    pieces += [(groups - batch, mid), (mid, groups)]
    for start, stop in pieces:
        receive(max(start, 1), stop).wait_recv()
        if start == batch:
            @pl.when(inner == 1)
            def _():
                for g in range(far - 1, 0, -1):
                    for p in members(g, True) + members(g, False):
                        send(p).start()
        score(start, stop)
    square = lax.broadcasted_iota(jnp.int32, (LANES, LANES), 0) == (
        lax.broadcasted_iota(jnp.int32, (LANES, LANES), 1)
    )
    for g in range(parts):
        span = slice(g * LANES, (g + 1) * LANES)
        top = jnp.max(best[span, :], axis=1, keepdims=True)
        row = jnp.max(jnp.where(square, top, -1.0), axis=0, keepdims=True)
        result[0, :, span] = jnp.maximum(result[0, :, span], row)

    def back(p):
        k = landed_from(p)
        return pltpu.make_async_remote_copy(
            src_ref=result.at[:, :, pl.ds(p // batch * LANES, LANES)],
            dst_ref=returned.at[pl.ds(k, 1)],
            send_sem=back_send_sem,
            recv_sem=back_recv_sem,
            device_id={"clu": me ^ k},
            device_id_type=pl.DeviceIdType.MESH,
        )

    def home():
        return pltpu.make_async_remote_copy(
            src_ref=returned.at[pl.ds(1, groups - 1)],
            dst_ref=returned.at[pl.ds(1, groups - 1)],
            send_sem=back_send_sem,
            recv_sem=back_recv_sem,
            device_id={"clu": me ^ SIDE},
            device_id_type=pl.DeviceIdType.MESH,
        )

    for p in range(groups - 1, 0, -1):
        back(p).start()
    returned[0] = result[0, :, 0:LANES]
    pltpu.make_async_remote_copy(
        src_ref=outgoing.at[pl.ds(block, total - block)],
        dst_ref=arrived.at[pl.ds(block, total - block)],
        send_sem=send_sem,
        recv_sem=recv_sem.at[0],
        device_id={"clu": me ^ SIDE},
        device_id_type=pl.DeviceIdType.MESH,
    ).wait_send()
    home().wait_recv()
    picked = jnp.broadcast_to(returned[0], (count, LANES))
    for k in range(1, groups):
        picked = jnp.where(peer_col == k, returned[k], picked)
    answer = jnp.sum(jnp.where(chosen, picked, 0.0), axis=1, keepdims=True)
    answer = jnp.sum(jnp.where(row_id == col_id, answer, 0.0), axis=0, keepdims=True)
    out_ref[...] = answer.reshape(out_ref.shape)
    home().wait_send()


def kernel_shards(embeddings, assignment):
    groups = lax.axis_size("clu")
    count, width = embeddings.shape
    most = 2 * count // (CLU_DEV * groups)
    total = CLU_DEV * groups * most
    pieces = total // LANES + 1
    return pl.pallas_call(
        functools.partial(exchange_kernel, groups, most),
        out_shape=pltpu.VMEM((count,), jnp.float32),
        in_specs=[
            pl.BlockSpec(memory_space=pl.ANY),
            pl.BlockSpec(memory_space=pl.ANY),
        ],
        out_specs=pl.BlockSpec(memory_space=pltpu.VMEM),
        scratch_shapes=[
            pltpu.VMEM((count, width), jnp.bfloat16),
            pltpu.VMEM((1, count), jnp.int32),
            pltpu.VMEM((total, width), jnp.bfloat16),
            pltpu.VMEM((total, width), jnp.bfloat16),
            pltpu.VMEM((total, LANES), jnp.float32),
            pltpu.VMEM((total, LANES), jnp.float32),
            pltpu.VMEM((1, 1, total), jnp.float32),
            pltpu.VMEM((groups, 1, LANES), jnp.float32),
            pltpu.SemaphoreType.DMA,
            pltpu.SemaphoreType.DMA,
            pltpu.SemaphoreType.DMA,
            pltpu.SemaphoreType.DMA((pieces,)),
            pltpu.SemaphoreType.DMA,
            pltpu.SemaphoreType.DMA,
            pltpu.SemaphoreType.REGULAR,
        ],
        compiler_params=pltpu.CompilerParams(collective_id=0, has_side_effects=True),
    )(embeddings, assignment.reshape(1, count))


def slot_index(cluster, groups, most):
    count = cluster.shape[0]
    order = jnp.argsort(cluster, stable=True)
    ranked = cluster[order]
    first = jnp.searchsorted(ranked, ranked, side="left")
    rank_sorted = jnp.arange(count, dtype=jnp.int32) - first
    rank = jnp.zeros((count,), jnp.int32).at[order].set(rank_sorted)
    local = cluster % CLU_DEV
    owner = cluster // CLU_DEV
    return (local * groups + owner) * most + rank


def cluster_scores(pieces):
    rows, flags = pieces
    items = rows.shape[0]
    width = rows.shape[1] * rows.shape[2]
    rows = rows.reshape(items, width, rows.shape[3])
    flags = flags.reshape(items, width)
    offsets = jnp.arange(width, dtype=jnp.int32)
    distinct = offsets[:, None] != offsets[None, :]

    def single(pair):
        block, marks = pair
        gram = lax.dot_general(
            block, block, (((1,), (1,)), ((), ())), preferred_element_type=jnp.float32
        )
        keep = distinct & (marks > 0)[None, :]
        best = jnp.max(jnp.where(keep, gram, jnp.float32(-2.0)), axis=1)
        return jnp.maximum(best, jnp.float32(-1.0))

    best = lax.map(single, (rows, flags))
    return best.reshape(items, 1, width)


def general_shards(embeddings, assignment):
    groups = lax.axis_size("clu")
    count = embeddings.shape[0]
    width = embeddings.shape[1]
    most = 2 * count // (CLU_DEV * groups)
    unit = normalize(embeddings)
    cluster = assignment[:, 0]
    slot = slot_index(cluster, groups, most)
    total = CLU_DEV * groups * most
    outgoing = jnp.zeros((total, width), jnp.bfloat16).at[slot].set(unit)
    marks = jnp.zeros((total,), jnp.bfloat16).at[slot].set(jnp.ones((count,), jnp.bfloat16))
    outgoing = outgoing.reshape(CLU_DEV, groups, most, width)
    marks = marks.reshape(CLU_DEV, groups, most)
    arrived = (
        lax.all_to_all(outgoing, "clu", split_axis=1, concat_axis=2, tiled=True),
        lax.all_to_all(marks, "clu", split_axis=1, concat_axis=2, tiled=True),
    )
    best = cluster_scores(arrived)
    returned = lax.all_to_all(best, "clu", split_axis=2, concat_axis=1, tiled=True)
    return returned.reshape(total)[slot]


def shards(embeddings, assignment):
    groups = lax.axis_size("clu")
    count = embeddings.shape[0]
    most = 2 * count // (CLU_DEV * groups)
    block = CLU_DEV * most
    power = groups & (groups - 1) == 0 and most & (most - 1) == 0
    if power and block % 16 == 0 and LANES % block == 0 and groups * block == 4 * LANES:
        return kernel_shards(embeddings, assignment)
    return general_shards(embeddings, assignment)


def solution(mesh):
    in_specs = (P(("lang", "clu"), None), P(("lang", "clu"), None))
    out_specs = P(("lang", "clu"))
    return jax.shard_map(shards, mesh=mesh, in_specs=in_specs, out_specs=out_specs, check_vma=False)
```
